256 devices in a mesh: energy: 32 (over y, z_lo, x), space: 8 (over z_hi, core).
Axes of the slice: x: 4, y: 4, z: 8 (z_hi: 4, z_lo: 2; z = z_hi * 2 + z_lo), core: 2. Of those that a mesh axis runs over, the one named last changes fastest.
Arguments:
- lesser: bfloat16 [64, 8, 2, 384, 384], P('energy', 'space'), may hold values from -6 to 6
- coupling: bfloat16 [8, 2, 384, 384], P('space'), may hold values from -0.21875 to 0.21875
- neighbours: int32 [8, 3], P('space'), may hold values from 0 to 7, as said below
- greater: bfloat16 [64, 8, 2, 384, 384], P(None, 'space', None, 'energy'), may hold values from -0.5 to 0.5
- closing: bfloat16 [8, 2, 384, 384], P('space'), may hold values from -0.21875 to 0.21875
Outputs:
- sigma: bfloat16 [64, 8, 2, 384, 384], P('energy', 'space')
The draws below stay inside these ranges and needn't reach their ends.
Inputs may be any that keep to these rules, and one draw needn't show every extreme that they name: `neighbours`: row i names only blocks i - 1, i and i + 1, clipped to 0 .. 7; every row other than the first and the last names both i - 1 and i + 1.
All inputs are finite; a program needn't handle non-finite values.
Results may differ from the reference program's by a relative error of at most 0.007.
Values may be sent and summed in bfloat16 or wider, within the bound.
No kernel may reach another device: no remote copies, remote signals or barrier semaphores. Data moves between devices by JAX's collectives and lax.ppermute only.
A program may use at most 64 MiB of HBM per device.

```python
import jax
import jax.numpy as jnp
from jax import lax

ORDER = 384
NE = 64
NB = 8


def draw_neighbours(key, part):
    positions = jnp.arange(NB, dtype=jnp.int32)
    side_sign = 2 * jax.random.randint(jax.random.fold_in(key, 11), (NB,), 0, 2, dtype=jnp.int32) - 1
    middle = positions + jax.random.randint(jax.random.fold_in(key, 12), (NB,), -1, 2, dtype=jnp.int32)
    table = jnp.stack([positions + side_sign, middle, positions - side_sign], axis=1)
    return jnp.clip(table, 0, NB - 1).astype(jnp.int32)


def block_levels(rng, dims, split, smallest, high):
    factor_of = 1.0
    for axis_at, blocks in split:
        draws = jax.random.uniform(jax.random.fold_in(jax.random.fold_in(rng, 6), axis_at), (blocks,), jnp.float32, smallest / len(split), high / len(split))
        factor_of = factor_of * jnp.repeat(jnp.exp(draws), dims[axis_at] // blocks).reshape((-1,) + (1,) * (len(dims) - 1 - axis_at))
    return factor_of


def bell_draw(stream_key, shape, scale, reach, cuts=(), held_as=jnp.bfloat16):
    level = block_levels(stream_key, shape, cuts, -0.22, 0.18) if cuts else 1.0
    entries = jax.random.normal(stream_key, shape, jnp.float32) * scale * level
    return jnp.minimum(jnp.maximum(entries, -reach), reach).astype(held_as)


def setup_inputs(seed: int = 0) -> dict:
    keys = jax.random.split(jax.random.key(seed), 6)
    lesser = bell_draw(keys[0], (NE, NB, 2, ORDER, ORDER), 1.0, 6.0, ((0, 32), (1, 8)))
    coupling = bell_draw(keys[1], (NB, 2, ORDER, ORDER), (2 * ORDER) ** -0.5, 0.21875, ((0, 8),))
    neighbours = draw_neighbours(jax.random.fold_in(keys[5], 71), 0)
    greater = bell_draw(keys[3], (NE, NB, 2, ORDER, ORDER), (2 * NE) ** -0.5, 0.5, ((1, 8), (3, 32)))
    closing = bell_draw(keys[4], (NB, 2, ORDER, ORDER), (2 * ORDER) ** -0.5, 0.21875, ((0, 8),))
    return {"lesser": lesser, "coupling": coupling, "neighbours": neighbours, "greater": greater, "closing": closing}


def round_half(value):
    return lax.optimization_barrier(value.astype(jnp.bfloat16)).astype(jnp.float32)


def left_product(left_real, left_imag, right_real, right_imag):
    def mult(a, b):
        return jnp.einsum('rs,est->ert', a, b, precision=lax.Precision.HIGHEST)
    return mult(left_real, right_real) - mult(left_imag, right_imag), mult(left_real, right_imag) + mult(left_imag, right_real)


def right_adjoint(left_real, left_imag, right_real, right_imag):
    def mult(a, b):
        return jnp.einsum('ers,ts->ert', a, b, precision=lax.Precision.HIGHEST)
    return mult(left_real, right_real) + mult(left_imag, right_imag), mult(left_imag, right_real) - mult(left_real, right_imag)


def reference(lesser, coupling, neighbours, greater, closing):
    def one_block(index):
        slab = lax.dynamic_index_in_dim(lesser, index, 1, False).astype(jnp.float32)
        table_row = lax.dynamic_index_in_dim(neighbours, index, 0, False)
        total_real = jnp.zeros((NE, ORDER, ORDER), jnp.float32)
        total_imag = jnp.zeros((NE, ORDER, ORDER), jnp.float32)
        for term in range(3):
            matrix = lax.dynamic_index_in_dim(coupling, table_row[term], 0, False).astype(jnp.float32)
            part_real, part_imag = left_product(matrix[0], matrix[1], slab[:, 0], slab[:, 1])
            part_real = round_half(part_real)
            part_imag = round_half(part_imag)
            add_real, add_imag = right_adjoint(part_real, part_imag, matrix[0], matrix[1])
            total_real = total_real + add_real
            total_imag = total_imag + add_imag
        screened = lax.dynamic_index_in_dim(greater, index, 1, False).astype(jnp.float32)
        left_complex = total_real + 1j * total_imag
        right_complex = screened[:, 0] + 1j * screened[:, 1]
        folded = jnp.fft.ifft(jnp.fft.fft(left_complex, axis=0) * jnp.fft.fft(right_complex, axis=0), axis=0)
        conv_real = round_half(jnp.real(folded))
        conv_imag = round_half(jnp.imag(folded))
        final = lax.dynamic_index_in_dim(closing, index, 0, False).astype(jnp.float32)
        mid_real, mid_imag = left_product(final[0], final[1], conv_real, conv_imag)
        mid_real = round_half(mid_real)
        mid_imag = round_half(mid_imag)
        out_real, out_imag = right_adjoint(mid_real, mid_imag, final[0], final[1])
        return jnp.stack([out_real, out_imag], axis=1).astype(jnp.bfloat16)

    result = lax.map(one_block, jnp.arange(NB, dtype=jnp.int32))
    return jnp.swapaxes(result, 0, 1)
```

```python
import math

import jax
import jax.numpy as jnp
import numpy as np
from jax import lax
from jax.experimental import pallas as pl
from jax.experimental.pallas import tpu as pltpu
from jax.sharding import PartitionSpec as P

F32 = jnp.float32
BF16 = jnp.bfloat16


def split_table(table):
    high = jnp.asarray(table, F32).astype(BF16)
    low = (jnp.asarray(table, F32) - high.astype(F32)).astype(BF16)
    return high, low


def forward_table(order):
    points = len(order) // 2
    freq = np.arange(points)[:, None]
    spot = np.array([e for e, _ in order])[None, :]
    part = np.array([p for _, p in order])[None, :]
    angle = 2.0 * math.pi * (freq * spot % points) / points
    cosine, sine = np.cos(angle), np.sin(angle)
    real = np.where(part == 0, cosine, sine)
    imag = np.where(part == 0, -sine, cosine)
    return np.concatenate([real, imag], axis=0)


def inverse_table(order):
    return forward_table(order).T / (len(order) // 2)


def dot(a, b):
    return lax.dot_general(a, b, (((1,), (0,)), ((), ())), preferred_element_type=F32)


def dot_nt(a, b):
    return lax.dot_general(a, b, (((1,), (1,)), ((), ())), preferred_element_type=F32)


def congruence(matrix, right, big, mid, emit):
    n = matrix.shape[-1]
    real, imag = matrix[0], matrix[1]
    big[:n, :n] = real
    big[:n, n:] = -imag
    big[n:, :n] = imag
    big[n:, n:] = real
    first = dot(big[...], right[...])
    for e in range(2):
        mid[e, :, :n] = first[:n, e * n : (e + 1) * n].astype(BF16)
        mid[e, :, n:] = (-first[n:, e * n : (e + 1) * n]).astype(BF16)
    for e in range(2):
        both = dot_nt(mid[e], big[...])
        emit(e, both[:, :n], -both[:, n:])


def count(names, block):
    total = jnp.int32(0)
    for k in range(3):
        total = total + (names[0, k] == block).astype(jnp.int32)
    return total.astype(F32)


def near_terms(names, here, slab, own, partner, out, right, big, mid):
    n = own.shape[-1]
    index = here[0]
    for e in range(2):
        for p in range(2):
            right[p * n : (p + 1) * n, e * n : (e + 1) * n] = slab[e, p]
    weight = count(names, index)

    def first(e, re, im):
        out[e, 0] = weight * re
        out[e, 1] = weight * im

    congruence(own, right, big, mid, first)
    weight_partner = count(names, index ^ 1)

    def second(e, re, im):
        out[e, 0] += weight_partner * re
        out[e, 1] += weight_partner * im

    congruence(partner, right, big, mid, second)


def far_term(names, here, slab, far, partial, out, right, big, mid, rows):
    n = far.shape[-1]
    index = here[0]
    for e in range(2):
        for p in range(2):
            right[p * n : (p + 1) * n, e * n : (e + 1) * n] = slab[e, p]
    weight = count(names, index + 2 * (index & 1) - 1)

    def add(e, re, im):
        for p, value in ((0, re), (1, im)):
            total = partial[e, p] + weight * value
            for j in range(n // 128):
                rows[j, pl.ds(2 * e + p, n, stride=4), :] = total[:, 128 * j : 128 * (j + 1)]

    congruence(far, right, big, mid, add)
    group = out.shape[1]
    for d in range(out.shape[0]):
        for j in range(n // 128):
            out[d, :, 128 * j : 128 * (j + 1)] = rows[j, d * group : (d + 1) * group, :].astype(BF16)


def screened_spectrum(greater, table, out, rows):
    points, _, held, n = greater.shape
    pitch = 16
    for j in range(n // 128):
        for e in range(points):
            for p in range(2):
                at = (2 * e + p) * pitch
                rows[j, at : at + held, :] = greater[e, p, :, 128 * j : 128 * (j + 1)].astype(F32)
    for r in range(held):
        for j in range(n // 128):
            line = rows[j, pl.ds(r, 2 * points, stride=pitch), :].astype(BF16)
            both = jnp.concatenate([line, line], axis=0)
            out[r, :, 128 * j : 128 * (j + 1)] = dot(table[...], both)


def convolve(arrived, spectrum, table, back, out, rows, result):
    peers, group, n = arrived.shape
    held = group // 4
    points = 2 * peers
    for d in range(peers):
        for j in range(n // 128):
            rows[j, d * group : (d + 1) * group, :] = arrived[d, :, 128 * j : 128 * (j + 1)].astype(F32)
    for r in range(held):
        for j in range(n // 128):
            line = jnp.concatenate(
                [rows[j, pl.ds(4 * r + q, peers, stride=group), :] for q in range(4)], axis=0
            ).astype(BF16)
            left = dot(table[...], jnp.concatenate([line, line], axis=0))
            other = spectrum[r, :, 128 * j : 128 * (j + 1)]
            left_re, left_im = left[:points], left[points:]
            right_re, right_im = other[:points], other[points:]
            prod = jnp.concatenate(
                [left_re * right_re - left_im * right_im, left_re * right_im + left_im * right_re],
                axis=0,
            )
            high = prod.astype(BF16)
            low = (prod - high.astype(F32)).astype(BF16)
            spot = dot(back[...], jnp.concatenate([high, low, high], axis=0))
            for q in range(4):
                result[j, pl.ds(4 * r + q, peers, stride=group), :] = spot[q * peers : (q + 1) * peers]
    for d in range(peers):
        for j in range(n // 128):
            out[d, :, 128 * j : 128 * (j + 1)] = result[j, d * group : (d + 1) * group, :].astype(BF16)


def finish(arrived, final, out, right, big, mid, rows):
    peers, group, n = arrived.shape
    for d in range(peers):
        for j in range(n // 128):
            rows[j, d * group : (d + 1) * group, :] = arrived[d, :, 128 * j : 128 * (j + 1)].astype(F32)
    for e in range(2):
        for p in range(2):
            for j in range(n // 128):
                at = e * n + 128 * j
                right[p * n : (p + 1) * n, at : at + 128] = rows[
                    j, pl.ds(2 * e + p, n, stride=4), :
                ].astype(BF16)

    def store(e, re, im):
        out[e, 0] = re.astype(BF16)
        out[e, 1] = im.astype(BF16)

    congruence(final, right, big, mid, store)


VMEM = pl.BlockSpec(memory_space=pltpu.VMEM)
SMEM = pl.BlockSpec(memory_space=pltpu.SMEM)


def work_space(n):
    return [
        pltpu.VMEM((2 * n, 2 * n), BF16),
        pltpu.VMEM((2 * n, 2 * n), BF16),
        pltpu.VMEM((2, n, 2 * n), BF16),
    ]


def call(body, name, out, in_specs, scratch, flops):
    return pl.pallas_call(
        body,
        name=name,
        out_shape=out,
        in_specs=in_specs,
        out_specs=VMEM,
        scratch_shapes=scratch,
        cost_estimate=pl.CostEstimate(flops=flops, bytes_accessed=4 << 20, transcendentals=0),
        compiler_params=pltpu.CompilerParams(vmem_limit_bytes=48 << 20),
    )


def local(lesser, coupling, neighbours, greater, closing):
    n = lesser.shape[-1]
    peers = lax.axis_size("energy")
    points = greater.shape[0]
    held = greater.shape[3]
    group = 4 * held
    blocks = lax.axis_size("space")
    slab = lesser[:, 0]
    own = coupling[0]
    partner = lax.ppermute(own, "space", [(i, i ^ 1) for i in range(blocks)])
    outward = [(i, i + 2 * (i & 1) - 1) for i in range(blocks)]
    far = lax.ppermute(own, "space", [(i, j) for i, j in outward if 0 <= j < blocks])
    here = lax.axis_index("space").astype(jnp.int32).reshape(1)

    order_w = [(e, p) for e in range(points) for p in range(2)]
    order_p = [(2 * d + q // 2, q % 2) for q in range(4) for d in range(peers)]
    table_w = jnp.concatenate(split_table(forward_table(order_w)), axis=1)
    table_p = jnp.concatenate(split_table(forward_table(order_p)), axis=1)
    back_high, back_low = split_table(inverse_table(order_p))
    table_b = jnp.concatenate([back_high, back_high, back_low], axis=1)

    flops = 4 * (2 * n) ** 3
    shuffled = pltpu.VMEM((n // 128, peers * group, 128), F32)
    spectrum = call(
        screened_spectrum,
        "screened_spectrum",
        jax.ShapeDtypeStruct((held, 2 * points, n), F32),
        [VMEM, VMEM],
        [pltpu.VMEM((n // 128, 2 * points * 16, 128), F32)],
        flops,
    )(greater[:, 0], table_w)
    partial = call(
        near_terms,
        "near_terms",
        jax.ShapeDtypeStruct((2, 2, n, n), F32),
        [SMEM, SMEM, VMEM, VMEM, VMEM],
        work_space(n),
        2 * flops,
    )(neighbours, here, slab, own, partner)
    chunks = jax.ShapeDtypeStruct((peers, group, n), BF16)
    sent = call(
        far_term,
        "far_term",
        chunks,
        [SMEM, SMEM, VMEM, VMEM, VMEM],
        work_space(n) + [shuffled],
        flops,
    )(neighbours, here, slab, far, partial)
    arrived = lax.all_to_all(sent, "energy", split_axis=0, concat_axis=0, tiled=True)
    convolved = call(
        convolve,
        "convolve",
        chunks,
        [VMEM, VMEM, VMEM, VMEM],
        [shuffled, shuffled],
        flops,
    )(arrived, spectrum, table_p, table_b)
    returned = lax.all_to_all(convolved, "energy", split_axis=0, concat_axis=0, tiled=True)
    sigma = call(
        finish,
        "finish",
        jax.ShapeDtypeStruct((2, 2, n, n), BF16),
        [VMEM, VMEM],
        work_space(n) + [shuffled],
        flops,
    )(returned, closing[0])
    return sigma[:, None]


def solution(mesh):
    placed = (
        P("energy", "space", None, None, None),
        P("space", None, None, None),
        P("space", None),
        P(None, "space", None, "energy", None),
        P("space", None, None, None),
    )
    return jax.shard_map(
        local,
        mesh=mesh,
        in_specs=placed,
        out_specs=P("energy", "space", None, None, None),
        check_vma=False,
    )
```
